32 devices in a mesh: rep: 4 (over y, core), grp: 8 (over z, x).
Axes of the slice: x: 2, y: 2, z: 4, core: 2. Of those that a mesh axis runs over, the one named last changes fastest.
Arguments:
- hidden_in: bfloat16 [128, 7168], P(('rep', 'grp')), may hold values from -3 to 3
- q_nope: bfloat16 [128, 8192], P(('rep', 'grp')), may hold values from -9 to 9
- q_rope: bfloat16 [128, 4096], P(('rep', 'grp')), may hold values from -36 to 36
- new_kv: bfloat16 [128, 576], P(('rep', 'grp')), may hold values from -6 to 6
- cache_kv: bfloat16 [128, 4096, 576], P(('rep', 'grp')), may hold values from -10 to 10
- lengths: int32 [128], P(('rep', 'grp')), may hold values from 2 to 4096, as said below
- w_uk: bfloat16 [512, 8192], P('rep'), may hold values from -0.5 to 0.5
- w_uv: bfloat16 [512, 8192], P('rep'), may hold values from -0.25 to 0.25
- w_out: bfloat16 [8192, 7168], P('grp'), may hold values from -0.0625 to 0.0625
- norm_gain: bfloat16 [7168], replicated, may hold values from 0.5 to 1.5
- w_gate: bfloat16 [7168, 18432], P(None, ('rep', 'grp')), may hold values from -0.0625 to 0.0625
- w_up: bfloat16 [7168, 18432], P(None, ('rep', 'grp')), may hold values from -0.0625 to 0.0625
- w_down: bfloat16 [18432, 7168], P(('rep', 'grp')), may hold values from -0.046875 to 0.046875
Outputs:
- hidden_out: bfloat16 [128, 7168], P(('rep', 'grp'))
The draws below stay inside these ranges and needn't reach their ends.
Inputs may be any that keep to these rules, and one draw needn't show every extreme that they name: `lengths`: every sequence has 2 or more cached positions and at most 4096; some sequence has exactly 4096.
All inputs are finite; a program needn't handle non-finite values.
Results may differ from the reference program's by a relative error of at most 0.03.
Values may be sent and summed in bfloat16 or wider, within the bound.
No kernel may reach another device: no remote copies, remote signals or barrier semaphores. Data moves between devices by JAX's collectives and lax.ppermute only.
A program may use at most 192 MiB of HBM per device.

```python
import jax
import jax.numpy as jnp
from jax import lax

D = 7168
FF = 18432
H = 64
NOPE = 128
ROPE = 64
VH = 128
KV_RANK = 512
CACHE = 4096
SEQS = 128


def draw_q_rope(key, part):
    values = jnp.clip(jax.random.normal(jax.random.fold_in(key, 3), (SEQS, H, ROPE), jnp.float32), -6.0, 6.0)
    return values.reshape(SEQS, H * ROPE).astype(jnp.bfloat16)


def draw_cache_kv(key, part):
    inner = jax.random.fold_in(key, 4)
    values = jnp.clip(jax.random.normal(inner, (SEQS, CACHE, KV_RANK + ROPE), jnp.float32), -6.0, 6.0)
    return values.astype(jnp.bfloat16)


def draw_lengths(key, part):
    inner = jax.random.fold_in(key, 5)
    lengths_drawn = jax.random.randint(inner, (SEQS,), 2, CACHE + 1, dtype=jnp.int32)
    where_full = jax.random.randint(jax.random.fold_in(inner, 6), (), 0, SEQS, dtype=jnp.int32)
    return jnp.where(jnp.arange(SEQS, dtype=jnp.int32) == where_full, CACHE, lengths_drawn).astype(jnp.int32)


def block_levels(key, shape, split, smallest, high):
    def one(position, shards_of):
        steps = jax.random.uniform(jax.random.fold_in(jax.random.fold_in(key, 6), position), (shards_of,), jnp.float32, smallest / len(split), high / len(split))
        return jnp.repeat(jnp.exp(steps), shape[position] // shards_of).reshape((-1,) + (1,) * (len(shape) - position - 1))

    loudness = one(*split[0])
    for cut in split[1:]:
        loudness = loudness * one(*cut)
    return loudness


def normal_values(stream_key, extent, scale, bound, pieces=(), kind=jnp.bfloat16):
    array = jax.random.normal(stream_key, extent, jnp.float32) * scale
    if len(pieces) > 0:
        array = block_levels(stream_key, extent, pieces, -0.22, 0.18) * array
    return jnp.clip(array, min=-bound, max=bound).astype(kind)


def setup_inputs(seed: int = 0) -> dict:
    key_list = jax.random.split(jax.random.key(seed), 14)
    return {
        "hidden_in": normal_values(key_list[0], (SEQS, D), 0.5, 3.0, ((0, 32),)),
        "q_nope": normal_values(key_list[1], (SEQS, H * NOPE), 1.5, 9.0, ((0, 32),)),
        "q_rope": draw_q_rope(jax.random.fold_in(key_list[13], 71), 0),
        "new_kv": normal_values(key_list[3], (SEQS, KV_RANK + ROPE), 1.0, 6.0, ((0, 32),)),
        "cache_kv": draw_cache_kv(jax.random.fold_in(key_list[13], 71), 0),
        "lengths": draw_lengths(jax.random.fold_in(key_list[13], 71), 0),
        "w_uk": normal_values(key_list[6], (KV_RANK, H * NOPE), NOPE ** -0.5, 0.5, ((0, 4),)),
        "w_uv": normal_values(key_list[7], (KV_RANK, H * VH), KV_RANK ** -0.5, 0.25, ((0, 4),)),
        "w_out": normal_values(key_list[8], (H * VH, D), (H * VH) ** -0.5, 0.0625, ((0, 8),)),
        "norm_gain": jnp.clip(1.0 + 0.1 * jax.random.normal(key_list[9], (D,), jnp.float32), 0.5, 1.5).astype(jnp.bfloat16),
        "w_gate": normal_values(key_list[10], (D, FF), D ** -0.5, 0.0625, ((1, 32),)),
        "w_up": normal_values(key_list[11], (D, FF), D ** -0.5, 0.0625, ((1, 32),)),
        "w_down": normal_values(key_list[12], (FF, D), FF ** -0.5, 0.046875, ((0, 32),)),
    }


epsilon = 1e-06

def norm_rows(resid, norm_gain):
    resid_f32 = resid.astype(jnp.float32)
    mean_sq = lax.optimization_barrier(jnp.mean(resid_f32 * resid_f32, axis=1, keepdims=True))
    return (resid_f32 * lax.rsqrt(mean_sq + epsilon) * norm_gain.astype(jnp.float32)).astype(jnp.bfloat16)

def reference(hidden_in, q_nope, q_rope, new_kv, cache_kv, lengths, w_uk, w_uv, w_out, norm_gain, w_gate, w_up, w_down):
    seq_count = hidden_in.shape[0]
    nope_part = q_nope.reshape(seq_count, H, NOPE).astype(jnp.float32)
    key_up = w_uk.reshape(KV_RANK, H, NOPE).astype(jnp.float32)
    q_lat = jnp.einsum('bhd,chd->bhc', nope_part, key_up).astype(jnp.bfloat16)
    queries = jnp.concatenate([q_lat, q_rope.reshape(seq_count, H, ROPE)], axis=2)
    score_scale = float(NOPE + ROPE) ** (-0.5)
    positions = jnp.arange(CACHE, dtype=jnp.int32)

    def attend(sequence_item):
        one_query, one_cache, one_new, one_length = sequence_item
        scores = jnp.dot(one_query, one_cache.T, preferred_element_type=jnp.float32) * score_scale
        scores = jnp.where(positions[None, :] < one_length, scores, -jnp.inf)
        own_score = jnp.dot(one_query, one_new, preferred_element_type=jnp.float32) * score_scale
        row_top = jnp.maximum(lax.optimization_barrier(jnp.max(scores, axis=1)), own_score)
        weights = jnp.exp(scores - row_top[:, None])
        own_weight = jnp.exp(own_score - row_top)
        denom_sum = lax.optimization_barrier(jnp.sum(weights, axis=1)) + own_weight
        softmax_w = (weights / denom_sum[:, None]).astype(jnp.bfloat16)
        own_prob = (own_weight / denom_sum).astype(jnp.bfloat16)
        mixture = jnp.dot(softmax_w, one_cache, preferred_element_type=jnp.float32)
        mixture = mixture + own_prob.astype(jnp.float32)[:, None] * one_new.astype(jnp.float32)[None, :]
        return mixture[:, :KV_RANK].astype(jnp.bfloat16)
    latent = lax.map(attend, (queries, cache_kv, new_kv, lengths))
    value_up = w_uv.reshape(KV_RANK, H, VH).astype(jnp.float32)
    head_out = jnp.einsum('bhc,che->bhe', latent.astype(jnp.float32), value_up).astype(jnp.bfloat16)
    attn_out = jnp.dot(head_out.reshape(seq_count, H * VH), w_out, preferred_element_type=jnp.float32)
    resid = (hidden_in.astype(jnp.float32) + attn_out).astype(jnp.bfloat16)
    normed = norm_rows(resid, norm_gain)
    gate_val = jnp.dot(normed, w_gate, preferred_element_type=jnp.float32)
    up_val = jnp.dot(normed, w_up, preferred_element_type=jnp.float32)
    activated = (jax.nn.silu(gate_val) * up_val).astype(jnp.bfloat16)
    mlp_out = jnp.dot(activated, w_down, preferred_element_type=jnp.float32)
    return (resid.astype(jnp.float32) + mlp_out).astype(jnp.bfloat16)
```

```python
import jax
import jax.numpy as jnp
from jax import lax
from jax.sharding import PartitionSpec as P

NOPE = 128
ROPE = 64
VH = 128

AXES = ("rep", "grp")
epsilon = 1e-06


def xor_move(value, axis, size, bit):
    return lax.ppermute(value, axis, [(i, i ^ bit) for i in range(size)])


def phases(rep_size, grp_size):
    out = []
    bit = grp_size
    low = 2 if grp_size > 2 else 1
    while bit > low:
        step = 4 if bit // 4 >= low else 2
        bit //= step
        out.append(("grp", grp_size, bit, step))
    if low == 2:
        out.append(("grp", grp_size, 1, 2))
    bit = rep_size
    while bit > 1:
        bit //= 2
        out.append(("rep", rep_size, bit, 2))
    return out


def gather_rows(rows, order):
    held = rows
    for axis, size, bit, ways in order:
        parts = [held] + [xor_move(held, axis, size, bit * k) for k in range(1, ways)]
        held = jnp.concatenate(parts, axis=0)
    return held


def scatter_sum(value, order):
    for axis, size, bit, ways in reversed(order):
        per = value.shape[0] // ways
        total = value[:per].astype(jnp.float32)
        for k in range(1, ways):
            moved = xor_move(
                value[k * per : (k + 1) * per].astype(jnp.bfloat16), axis, size, bit * k
            )
            total = total + moved.astype(jnp.float32)
        value = total
    return value


def gather_in_order(rows, axis, size):
    me = lax.axis_index(axis)
    held, slots = [rows], [0]
    bit = size
    while bit > 1:
        bit //= 2
        here = (me & bit) == 0
        own = jnp.concatenate(held, axis=0)
        other = xor_move(own, axis, size, bit)
        low = jnp.split(jnp.where(here, own, other), len(held), axis=0)
        high = jnp.split(jnp.where(here, other, own), len(held), axis=0)
        held, slots = low + high, slots + [slot + bit for slot in slots]
    return jnp.concatenate([held[slots.index(i)] for i in range(size)], axis=0)


def on_device(
    hidden_in,
    q_nope,
    q_rope,
    new_kv,
    cache_kv,
    lengths,
    w_uk,
    w_uv,
    w_out,
    norm_gain,
    w_gate,
    w_up,
    w_down,
    *,
    rep_size,
    grp_size,
):
    seqs, width = hidden_in.shape
    heads = q_nope.shape[1] // NOPE
    capacity = cache_kv.shape[1]
    rank_own = w_uk.shape[0]
    rank = rank_own * rep_size
    own_heads = heads // grp_size

    value_own = lax.dynamic_slice_in_dim(
        w_uv, lax.axis_index("grp") * own_heads * VH, own_heads * VH, 1
    )

    q_all = lax.all_gather(q_nope, "rep", axis=0, tiled=True)
    q_part = jnp.einsum(
        "bhd,chd->bhc",
        q_all.reshape(seqs * rep_size, heads, NOPE),
        w_uk.reshape(rank_own, heads, NOPE),
        preferred_element_type=jnp.float32,
    ).astype(jnp.bfloat16)
    q_lat = lax.all_to_all(q_part, "rep", split_axis=0, concat_axis=2, tiled=True)

    value_up = gather_in_order(value_own, "rep", rep_size)

    queries = jnp.concatenate([q_lat, q_rope.reshape(seqs, heads, ROPE)], axis=2)
    score_scale = float(NOPE + ROPE) ** (-0.5)
    scores = (
        jnp.einsum("bhc,blc->bhl", queries, cache_kv, preferred_element_type=jnp.float32)
        * score_scale
    )
    positions = lax.broadcasted_iota(jnp.int32, (1, 1, capacity), 2)
    scores = jnp.where(positions < lengths[:, None, None], scores, -jnp.inf)
    own_score = (
        jnp.einsum("bhc,bc->bh", queries, new_kv, preferred_element_type=jnp.float32) * score_scale
    )
    row_top = jnp.maximum(jnp.max(scores, axis=2), own_score)
    weights = jnp.exp(scores - row_top[:, :, None])
    own_weight = jnp.exp(own_score - row_top)
    denom_sum = jnp.sum(weights, axis=2) + own_weight
    softmax_w = (weights / denom_sum[:, :, None]).astype(jnp.bfloat16)
    own_prob = (own_weight / denom_sum).astype(jnp.bfloat16)
    mixture = jnp.einsum("bhl,blc->bhc", softmax_w, cache_kv, preferred_element_type=jnp.float32)
    mixture = (
        mixture + own_prob.astype(jnp.float32)[:, :, None] * new_kv.astype(jnp.float32)[:, None, :]
    )
    latent = mixture[:, :, :rank].astype(jnp.bfloat16)

    regrouped = lax.all_to_all(latent, "grp", split_axis=1, concat_axis=0, tiled=True)
    head_out = jnp.einsum(
        "bhc,che->bhe",
        regrouped,
        value_up.reshape(rank, own_heads, VH),
        preferred_element_type=jnp.float32,
    ).astype(jnp.bfloat16)
    partial = jnp.dot(
        head_out.reshape(seqs * grp_size, -1), w_out, preferred_element_type=jnp.float32
    ).astype(jnp.bfloat16)
    pieces = lax.all_to_all(
        partial, "grp", split_axis=0, concat_axis=0, tiled=True
    ).reshape(grp_size, seqs, width)
    resid = (
        hidden_in.astype(jnp.float32) + jnp.sum(pieces.astype(jnp.float32), axis=0)
    ).astype(jnp.bfloat16)
    resid_f32 = resid.astype(jnp.float32)
    mean_sq = jnp.mean(resid_f32 * resid_f32, axis=1, keepdims=True)
    normed = (
        resid_f32 * lax.rsqrt(mean_sq + epsilon) * norm_gain.astype(jnp.float32)
    ).astype(jnp.bfloat16)

    order = phases(rep_size, grp_size)
    rows_in = gather_rows(normed, order)
    gate_val = jnp.dot(rows_in, w_gate, preferred_element_type=jnp.float32)
    up_val = jnp.dot(rows_in, w_up, preferred_element_type=jnp.float32)
    activated = (jax.nn.silu(gate_val) * up_val).astype(jnp.bfloat16)
    mlp_out = scatter_sum(
        jnp.dot(activated, w_down, preferred_element_type=jnp.float32), order
    )
    return (resid_f32 + mlp_out).astype(jnp.bfloat16)


def solution(mesh):
    def body(*args):
        return on_device(*args, rep_size=mesh.shape["rep"], grp_size=mesh.shape["grp"])

    return jax.shard_map(
        body,
        mesh=mesh,
        in_specs=(
            P(AXES, None),
            P(AXES, None),
            P(AXES, None),
            P(AXES, None),
            P(AXES, None, None),
            P(AXES),
            P("rep", None),
            P("rep", None),
            P("grp", None),
            P(),
            P(None, AXES),
            P(None, AXES),
            P(AXES, None),
        ),
        out_specs=P(AXES, None),
        check_vma=False,
    )
```

```python
import functools

import jax
import jax.numpy as jnp
from jax import lax
from jax.experimental import pallas as pl
from jax.experimental.pallas import tpu as pltpu
from jax.sharding import PartitionSpec as P

NOPE = 128
ROPE = 64
VH = 128

AXES = ("rep", "grp")
epsilon = 1e-06


MIB = 1024 * 1024
IN_HBM = pl.BlockSpec(memory_space=pltpu.HBM)
IN_VMEM = pl.BlockSpec(memory_space=pltpu.VMEM)
IN_SMEM = pl.BlockSpec(memory_space=pltpu.SMEM)
NT = (((1,), (1,)), ((), ()))


def chunk_of(size, wanted):
    chunk = wanted
    while size % chunk:
        chunk //= 2
    return chunk


def attend_kernel(
    lengths, place, *refs, chunk, scale
):
    pieces = refs[: place.shape[0]]
    q_rope, new_kv, cache_hbm, out, cache, queries, scores, total, sems = refs[place.shape[0] :]
    seqs, heads, own_rank = pieces[0].shape
    rank = own_rank * len(pieces)
    depth, capacity = cache.shape[1:]

    def part(i):
        return pl.ds(pl.multiple_of(i * chunk, chunk), chunk)

    def used(b):
        return (lengths[b] + (chunk - 1)) // chunk

    def copy(b, i):
        return pltpu.make_async_copy(
            cache_hbm.at[b, :, part(i)], cache.at[b, :, part(i)], sems.at[b, i]
        )

    for b in range(seqs):

        @pl.loop(0, used(b))
        def _(i):
            copy(b, i).start()

    for b in range(seqs):
        for j, piece in enumerate(pieces):
            columns = pl.ds(pl.multiple_of(place[j] * own_rank, own_rank), own_rank)
            queries[b, :, columns] = piece[b]
        queries[b, :, rank:] = q_rope[b]

    steps = used(0)
    for b in range(1, seqs):
        steps = steps + used(b)
    copy(0, 0).wait()
    scores[0] = jnp.dot(queries[0], cache[0, :, part(0)], preferred_element_type=jnp.float32)

    def step(t, carry):
        b, i, top, denom = carry
        slot = t & 1
        last = i + 1 == used(b)
        next_b = jnp.where(last, b + 1, b)
        next_i = jnp.where(last, 0, i + 1)

        @pl.when(t + 1 < steps)
        def _():
            copy(next_b, next_i).wait()

        ahead_b = jnp.minimum(next_b, seqs - 1)
        first = i == 0
        own = new_kv[b].astype(jnp.float32)
        own_score = jnp.sum(queries[b].astype(jnp.float32) * own, axis=1, keepdims=True)
        top = jnp.where(first, own_score, top)
        denom = jnp.where(first, 1.0, denom)
        ahead = jnp.dot(
            queries[ahead_b], cache[ahead_b, :, part(next_i)], preferred_element_type=jnp.float32
        )
        position = i * chunk + lax.broadcasted_iota(jnp.int32, (1, chunk), 1)
        raw = scores[slot] + jnp.where(position < lengths[b], 0.0, -jnp.inf)
        new_top = jnp.maximum(top, jnp.max(raw, axis=1, keepdims=True))
        weights = jnp.exp((raw - new_top) * scale)
        shrink = jnp.exp((top - new_top) * scale)
        denom = denom * shrink + jnp.sum(weights, axis=1, keepdims=True)
        before = jnp.where(first, jnp.broadcast_to(own[:, :rank], (heads, rank)), total[...])
        fresh = before * shrink + lax.dot_general(
            weights.astype(jnp.bfloat16),
            cache[b, :rank, part(i)],
            NT,
            preferred_element_type=jnp.float32,
        )
        scores[1 - slot] = ahead
        total[...] = fresh

        @pl.when(last)
        def _():
            out[b] = (fresh / denom).astype(out.dtype)

        return next_b, next_i, new_top, denom

    zero = jnp.zeros((heads, 1), jnp.float32)
    lax.fori_loop(0, steps, step, (jnp.int32(0), jnp.int32(0), zero, zero))


def attend(lengths, place, pieces, q_rope, new_kv, cache_kv, scale):
    seqs, heads, own_rank = pieces[0].shape
    rank = own_rank * len(pieces)
    capacity, depth = cache_kv.shape[1:]
    chunk = chunk_of(capacity, 1024)
    return pl.pallas_call(
        functools.partial(attend_kernel, chunk=chunk, scale=scale),
        out_shape=jax.ShapeDtypeStruct((seqs, heads, rank), jnp.bfloat16),
        in_specs=[IN_SMEM, IN_SMEM] + [IN_VMEM] * (len(pieces) + 2) + [IN_HBM],
        out_specs=IN_VMEM,
        scratch_shapes=[
            pltpu.VMEM((seqs, depth, capacity), jnp.bfloat16),
            pltpu.VMEM((seqs, heads, depth), jnp.bfloat16),
            pltpu.VMEM((2, heads, chunk), jnp.float32),
            pltpu.VMEM((heads, rank), jnp.float32),
            pltpu.SemaphoreType.DMA((seqs, capacity // chunk)),
        ],
        compiler_params=pltpu.CompilerParams(vmem_limit_bytes=50 * MIB),
        cost_estimate=pl.CostEstimate(
            flops=4 * seqs * heads * capacity * depth,
            bytes_accessed=2 * seqs * capacity * depth,
            transcendentals=seqs * heads * capacity,
        ),
        name="attend",
    )(lengths, place, *pieces, q_rope, new_kv[:, None, :], cache_kv.transpose(0, 2, 1))


def out_kernel(heads, weight_hbm, out, weight, sems, *, chunk):
    count = out.shape[1] // chunk

    def part(i):
        return pl.ds(pl.multiple_of(i * chunk, chunk), chunk)

    def copy(i):
        return pltpu.make_async_copy(weight_hbm.at[:, part(i)], weight.at[:, part(i)], sems.at[i])

    @pl.loop(0, count)
    def _(i):
        copy(i).start()

    @pl.loop(0, count)
    def _(i):
        copy(i).wait()
        out[:, part(i)] = jnp.dot(
            heads[...], weight[:, part(i)], preferred_element_type=jnp.float32
        ).astype(out.dtype)


def out_proj(heads, w_out):
    depth, width = w_out.shape
    chunk = chunk_of(width, 1024)
    return pl.pallas_call(
        functools.partial(out_kernel, chunk=chunk),
        out_shape=jax.ShapeDtypeStruct((heads.shape[0], width), jnp.bfloat16),
        in_specs=[IN_VMEM, IN_HBM],
        out_specs=IN_VMEM,
        scratch_shapes=[
            pltpu.VMEM((depth, width), jnp.bfloat16),
            pltpu.SemaphoreType.DMA((width // chunk,)),
        ],
        compiler_params=pltpu.CompilerParams(vmem_limit_bytes=54 * MIB),
        cost_estimate=pl.CostEstimate(
            flops=2 * heads.shape[0] * width * depth,
            bytes_accessed=2 * depth * width,
            transcendentals=0,
        ),
        name="out_proj",
    )(heads, w_out)


def mlp_kernel(
    own_low, own_high, other_low, other_high, gate_hbm, up_hbm, down_hbm,
    keep_low, keep_high, send,
    gate, up, down, gate_sum, up_sum, active, sems, *, chunk
):
    half, middle = own_low.shape
    count = middle // chunk

    def part(i):
        return pl.ds(pl.multiple_of(i * chunk, chunk), chunk)

    def copies(i):
        return (
            pltpu.make_async_copy(gate_hbm.at[:, part(i)], gate.at[:, part(i)], sems.at[0, i]),
            pltpu.make_async_copy(up_hbm.at[:, part(i)], up.at[:, part(i)], sems.at[1, i]),
        )

    def down_copy(i):
        return pltpu.make_async_copy(down_hbm.at[:, part(i)], down.at[:, part(i)], sems.at[2, i])

    @pl.loop(0, 2 * count)
    def _(i):
        for copy in copies(i):
            copy.start()

    @pl.loop(0, 2 * count)
    def _(i):
        down_copy(i).start()

    gate_sum[...] = jnp.zeros_like(gate_sum)
    up_sum[...] = jnp.zeros_like(up_sum)
    for side, (own, other) in enumerate(((own_low, other_low), (own_high, other_high))):

        @pl.loop(0, count)
        def _(i):
            rows = jnp.concatenate([own[:, part(i)], other[:, part(i)]], axis=0)
            gate_copy, up_copy = copies(i + side * count)
            gate_copy.wait()
            columns = part(i + side * count)
            gate_sum[...] += lax.dot_general(
                gate[:, columns], rows, NT, preferred_element_type=jnp.float32
            )
            up_copy.wait()
            up_sum[...] += lax.dot_general(
                up[:, columns], rows, NT, preferred_element_type=jnp.float32
            )

    value = gate_sum[...]
    active[...] = (value / (1.0 + jnp.exp(-value)) * up_sum[...]).T.astype(jnp.bfloat16)
    for side, keep in enumerate((keep_low, keep_high)):

        @pl.loop(0, count)
        def _(i):
            down_copy(i + side * count).wait()
            columns = part(i + side * count)
            result = jnp.dot(active[...], down[:, columns], preferred_element_type=jnp.float32)
            keep[:, part(i)] = result[:half].astype(keep.dtype)
            send[:, columns] = result[half:].astype(send.dtype)


def gated_mlp(own, other, w_gate, w_up, w_down):
    half, middle = own[0].shape
    hidden, width = w_down.shape
    chunk = chunk_of(middle, 1792)
    count = width // chunk
    return pl.pallas_call(
        functools.partial(mlp_kernel, chunk=chunk),
        out_shape=(
            jax.ShapeDtypeStruct((half, middle), jnp.float32),
            jax.ShapeDtypeStruct((half, middle), jnp.float32),
            jax.ShapeDtypeStruct((half, width), jnp.bfloat16),
        ),
        in_specs=[IN_VMEM] * 4 + [IN_HBM] * 3,
        out_specs=(IN_VMEM,) * 3,
        scratch_shapes=[
            pltpu.VMEM((hidden, width), jnp.bfloat16),
            pltpu.VMEM((hidden, width), jnp.bfloat16),
            pltpu.VMEM((hidden, width), jnp.bfloat16),
            pltpu.VMEM((hidden, 2 * half), jnp.float32),
            pltpu.VMEM((hidden, 2 * half), jnp.float32),
            pltpu.VMEM((2 * half, hidden), jnp.bfloat16),
            pltpu.SemaphoreType.DMA((3, count)),
        ],
        compiler_params=pltpu.CompilerParams(vmem_limit_bytes=57 * MIB),
        cost_estimate=pl.CostEstimate(
            flops=12 * half * width * hidden,
            bytes_accessed=6 * hidden * width,
            transcendentals=2 * half * hidden,
        ),
        name="gated_mlp",
    )(*own, *other, w_gate.T, w_up.T, w_down)


def direct_phases(rep_size, grp_size):
    out = []
    for axis, size, low in (("grp", grp_size, 2), ("rep", rep_size, 4)):
        bit = size
        while bit > low:
            ways = 4 if bit // 4 >= low else 2
            bit //= ways
            out.append((axis, size, bit, ways))
    return out


def gather_rows(rows, move, sizes):
    held = rows
    for axis, size, bit, ways in direct_phases(*sizes):
        held = jnp.concatenate([held] + [move(held, axis, bit * k) for k in range(1, ways)], axis=0)
    n, width = held.shape
    low, high = held[:, : width // 2], held[:, width // 2 :]
    low_x, high_y = move(low, "grp", 1), move(high, "rep", 2)
    low = jnp.concatenate([low, low_x], axis=0)
    wide = jnp.concatenate([high, high_y], axis=0)
    low_y, high_x = move(low, "rep", 2), move(wide, "grp", 1)
    low = jnp.concatenate([low, low_y], axis=0)
    high = jnp.concatenate([high, high_x[:n], high_y, high_x[n:]], axis=0)
    return (low, high), (move(low, "rep", 1), move(high, "rep", 1))


def scatter_sum(low, high, send, move, sizes):
    def add(mine, theirs):
        return mine + theirs.astype(jnp.float32)

    def narrow(value):
        return value.astype(jnp.bfloat16)

    middle = low.shape[1]
    n = low.shape[0] // 4
    got = move(send, "rep", 1)
    low, high = add(low, got[:, :middle]), add(high, got[:, middle:])
    low_got = move(narrow(low[2 * n :]), "rep", 2)
    high_got = move(narrow(jnp.concatenate([high[n : 2 * n], high[3 * n :]], axis=0)), "grp", 1)
    low = add(low[: 2 * n], low_got)
    high = add(jnp.concatenate([high[:n], high[2 * n : 3 * n]], axis=0), high_got)
    low_got, high_got = move(narrow(low[n:]), "grp", 1), move(narrow(high[n:]), "rep", 2)
    total = jnp.concatenate([add(low[:n], low_got), add(high[:n], high_got)], axis=1)
    for axis, size, bit, ways in reversed(direct_phases(*sizes)):
        per = total.shape[0] // ways
        moved = [
            move(narrow(total[k * per : (k + 1) * per]), axis, bit * k) for k in range(1, ways)
        ]
        total = total[:per]
        for piece in moved:
            total = add(total, piece)
    return total


def gather_in_order(rows, axis, size, move):
    me = lax.axis_index(axis)
    held, slots = [rows], [0]
    bit = size
    while bit > 1:
        bit //= 2
        here = (me & bit) == 0
        own = jnp.concatenate(held, axis=0)
        other = move(own, axis, bit)
        low = jnp.split(jnp.where(here, own, other), len(held), axis=0)
        high = jnp.split(jnp.where(here, other, own), len(held), axis=0)
        held, slots = low + high, slots + [slot + bit for slot in slots]
    return jnp.concatenate([held[slots.index(i)] for i in range(size)], axis=0)


def on_device(
    hidden_in,
    q_nope,
    q_rope,
    new_kv,
    cache_kv,
    lengths,
    w_uk,
    w_uv,
    w_out,
    norm_gain,
    w_gate,
    w_up,
    w_down,
    *,
    rep_size,
    grp_size,
):
    sizes = {"rep": rep_size, "grp": grp_size}

    def move(value, axis, bit):
        return lax.ppermute(value, axis, [(i, i ^ bit) for i in range(sizes[axis])])

    seqs, width = hidden_in.shape
    heads = q_nope.shape[1] // NOPE
    rank_own = w_uk.shape[0]
    rank = rank_own * rep_size
    own_heads = heads // grp_size

    held, steps_of = q_nope, [0]
    bit = rep_size
    while bit > 1:
        bit //= 2
        held = jnp.concatenate([held, move(held, "rep", bit)], axis=0)
        steps_of = steps_of + [step ^ bit for step in steps_of]
    q_part = jnp.einsum(
        "bhd,chd->bhc",
        held.reshape(seqs * rep_size, heads, NOPE),
        w_uk.reshape(rank_own, heads, NOPE),
        preferred_element_type=jnp.float32,
    ).astype(jnp.bfloat16)
    pieces = []
    for step in range(rep_size):
        at = steps_of.index(step) * seqs
        piece = q_part[at : at + seqs]
        pieces.append(move(piece, "rep", step) if step else piece)
    place = lax.axis_index("rep") ^ jnp.arange(rep_size, dtype=jnp.int32)

    value_own = lax.dynamic_slice_in_dim(
        w_uv, lax.axis_index("grp") * own_heads * VH, own_heads * VH, 1
    )
    value_up = gather_in_order(value_own, "rep", rep_size, move)

    latent = attend(
        lengths,
        place,
        pieces,
        q_rope.reshape(seqs, heads, ROPE),
        new_kv,
        cache_kv,
        float(NOPE + ROPE) ** (-0.5),
    )

    regrouped = lax.all_to_all(latent, "grp", split_axis=1, concat_axis=0, tiled=True)
    head_out = jnp.einsum(
        "bhc,che->bhe",
        regrouped,
        value_up.reshape(rank, own_heads, VH),
        preferred_element_type=jnp.float32,
    ).astype(jnp.bfloat16)
    partial = out_proj(head_out.reshape(seqs * grp_size, -1), w_out)
    parts = lax.all_to_all(partial, "grp", split_axis=0, concat_axis=0, tiled=True).reshape(
        grp_size, seqs, width
    )
    resid = (
        hidden_in.astype(jnp.float32) + jnp.sum(parts.astype(jnp.float32), axis=0)
    ).astype(jnp.bfloat16)
    resid_f32 = resid.astype(jnp.float32)
    mean_sq = jnp.mean(resid_f32 * resid_f32, axis=1, keepdims=True)
    normed = (
        resid_f32 * lax.rsqrt(mean_sq + epsilon) * norm_gain.astype(jnp.float32)
    ).astype(jnp.bfloat16)

    own, other = gather_rows(normed, move, (rep_size, grp_size))
    low, high, send = gated_mlp(own, other, w_gate, w_up, w_down)
    mlp_out = scatter_sum(low, high, send, move, (rep_size, grp_size))
    return (resid_f32 + mlp_out).astype(jnp.bfloat16)


def solution(mesh):
    def body(*args):
        return on_device(*args, rep_size=mesh.shape["rep"], grp_size=mesh.shape["grp"])

    return jax.shard_map(
        body,
        mesh=mesh,
        in_specs=(
            P(AXES, None),
            P(AXES, None),
            P(AXES, None),
            P(AXES, None),
            P(AXES, None, None),
            P(AXES),
            P("rep", None),
            P("rep", None),
            P("grp", None),
            P(),
            P(None, AXES),
            P(None, AXES),
            P(AXES, None),
        ),
        out_specs=P(AXES, None),
        check_vma=False,
    )
```

```python
import functools

import jax
import jax.numpy as jnp
from jax import lax
from jax.experimental import pallas as pl
from jax.experimental.pallas import tpu as pltpu
from jax.sharding import PartitionSpec as P


NOPE = 128
ROPE = 64
VH = 128

AXES = ("rep", "grp")
epsilon = 1e-06


MIB = 1024 * 1024
IN_HBM = pl.BlockSpec(memory_space=pltpu.HBM)
IN_VMEM = pl.BlockSpec(memory_space=pltpu.VMEM)
IN_SMEM = pl.BlockSpec(memory_space=pltpu.SMEM)
NT = (((1,), (1,)), ((), ()))


def chunk_of(size, wanted):
    chunk = wanted
    while size % chunk:
        chunk //= 2
    return chunk


def attend_kernel(lengths, place, group, *refs, chunk, scale, whole):
    pieces = refs[: place.shape[0]]
    (
        q_rope, new_kv, cache_hbm, weight_hbm, near, far, weight, cache, queries, scores, total,
        sems, weight_sems,
    ) = refs[place.shape[0] :]
    weight_rows = weight.shape[0] // weight_sems.shape[0]
    weight_copies = [
        pltpu.make_async_copy(
            weight_hbm.at[pl.ds(i * weight_rows, weight_rows)],
            weight.at[pl.ds(i * weight_rows, weight_rows)],
            weight_sems.at[i],
        )
        for i in range(weight_sems.shape[0])
    ]
    seqs, heads, own_rank = pieces[0].shape
    rank = own_rank * len(pieces)

    def part(i):
        return pl.ds(pl.multiple_of(i * chunk, chunk), chunk)

    def used(b):
        return (lengths[b] + (chunk - 1)) // chunk

    def copy(b, i):
        return pltpu.make_async_copy(
            cache_hbm.at[b, :, part(i)], cache.at[b, :, part(i)], sems.at[b, i]
        )

    for b in range(seqs):

        @pl.loop(0, used(b))
        def _(i):
            copy(b, i).start()

    for weight_copy in weight_copies:
        weight_copy.start()

    for b in range(seqs):
        for j, piece in enumerate(pieces):
            columns = pl.ds(pl.multiple_of(place[j] * own_rank, own_rank), own_rank)
            queries[b, :, columns] = piece[b]
        queries[b, :, rank:] = q_rope[b]

    steps = used(0)
    for b in range(1, seqs):
        steps = steps + used(b)
    copy(0, 0).wait()
    scores[0] = jnp.dot(queries[0], cache[0, :, part(0)], preferred_element_type=jnp.float32)

    def step(t, carry):
        b, i, top, denom = carry
        slot = t & 1
        last = i + 1 == used(b)
        next_b = jnp.where(last, b + 1, b)
        next_i = jnp.where(last, 0, i + 1)

        @pl.when(t + 1 < steps)
        def _():
            copy(next_b, next_i).wait()

        ahead_b = jnp.minimum(next_b, seqs - 1)
        first = i == 0
        own = new_kv[b].astype(jnp.float32)
        own_score = jnp.sum(queries[b].astype(jnp.float32) * own, axis=1, keepdims=True)
        top = jnp.where(first, own_score, top)
        denom = jnp.where(first, 1.0, denom)
        ahead = jnp.dot(
            queries[ahead_b], cache[ahead_b, :, part(next_i)], preferred_element_type=jnp.float32
        )
        position = i * chunk + lax.broadcasted_iota(jnp.int32, (1, chunk), 1)
        raw = scores[slot] + jnp.where(position < lengths[b], 0.0, -jnp.inf)
        new_top = jnp.maximum(top, jnp.max(raw, axis=1, keepdims=True))
        weights = jnp.exp((raw - new_top) * scale)
        shrink = jnp.exp((top - new_top) * scale)
        denom = denom * shrink + jnp.sum(weights, axis=1, keepdims=True)
        before = jnp.where(first, jnp.broadcast_to(own[:, :rank], (heads, rank)), total[...])
        fresh = before * shrink + lax.dot_general(
            weights.astype(jnp.bfloat16),
            cache[b, :rank, part(i)],
            NT,
            preferred_element_type=jnp.float32,
        )
        scores[1 - slot] = ahead
        total[...] = fresh

        @pl.when(last)
        def _():
            if whole:
                near[b] = (fresh / denom).astype(near.dtype)
                return
            total[...] = fresh / denom
            own_heads = heads // (2 * near.shape[0])
            place_rows = pl.ds(pl.multiple_of(b * own_heads, own_heads), own_heads)
            for x, block in enumerate((near, far)):
                for high in range(near.shape[0]):
                    first_head = (group[0] ^ (2 * high + x)) * own_heads
                    rows = pl.ds(pl.multiple_of(first_head, own_heads), own_heads)
                    block[high, place_rows, :] = total[rows, :].astype(block.dtype)

        return next_b, next_i, new_top, denom

    zero = jnp.zeros((heads, 1), jnp.float32)
    lax.fori_loop(0, steps, step, (jnp.int32(0), jnp.int32(0), zero, zero))
    for weight_copy in weight_copies:
        weight_copy.wait()


def attend(
    lengths, place, group, pieces, q_rope, new_kv, cache_kv, w_out, scale, grp_size
):
    seqs, heads, own_rank = pieces[0].shape
    rank = own_rank * len(pieces)
    capacity, depth = cache_kv.shape[1:]
    chunk = chunk_of(capacity, 1024)
    own_heads = heads // grp_size
    whole = own_heads % 8 != 0
    shapes = [(grp_size // 2, seqs * own_heads, rank)] * 2
    if whole:
        shapes = [(seqs, heads, rank), (8, 128)]
    blocks = [jax.ShapeDtypeStruct(shape, jnp.bfloat16) for shape in shapes]
    near, far, out_weight = pl.pallas_call(
        functools.partial(attend_kernel, chunk=chunk, scale=scale, whole=whole),
        out_shape=(*blocks, jax.ShapeDtypeStruct(w_out.shape, w_out.dtype)),
        in_specs=[IN_SMEM] * 3 + [IN_VMEM] * (len(pieces) + 2) + [IN_HBM] * 2,
        out_specs=(IN_VMEM,) * 3,
        scratch_shapes=[
            pltpu.VMEM((seqs, depth, capacity), jnp.bfloat16),
            pltpu.VMEM((seqs, heads, depth), jnp.bfloat16),
            pltpu.VMEM((2, heads, chunk), jnp.float32),
            pltpu.VMEM((heads, rank), jnp.float32),
            pltpu.SemaphoreType.DMA((seqs, capacity // chunk)),
            pltpu.SemaphoreType.DMA((4,)),
        ],
        compiler_params=pltpu.CompilerParams(vmem_limit_bytes=30 * MIB),
        cost_estimate=pl.CostEstimate(
            flops=4 * seqs * heads * capacity * depth,
            bytes_accessed=2 * seqs * capacity * depth,
            transcendentals=seqs * heads * capacity,
        ),
        name="attend",
    )(lengths, place, group, *pieces, q_rope, new_kv[:, None, :], cache_kv.transpose(0, 2, 1), w_out)
    if whole:
        latent = near.reshape(seqs, grp_size, own_heads, rank).swapaxes(0, 1)
        latent = latent.reshape(grp_size, seqs * own_heads, rank)
        latent = jnp.take(latent, group[0] ^ jnp.arange(grp_size), axis=0)
        near, far = latent[0::2], latent[1::2]
    return near, far, out_weight


def slice_kernel(start, source, out, sem):
    width = out.shape[1]
    columns = pl.ds(pl.multiple_of(start[0] * width, width), width)
    copy = pltpu.make_async_copy(source.at[:, columns], out, sem)
    copy.start()
    copy.wait()


def own_columns(source, index, width):
    return pl.pallas_call(
        slice_kernel,
        out_shape=jax.ShapeDtypeStruct((source.shape[0], width), source.dtype),
        in_specs=[IN_SMEM, IN_HBM],
        out_specs=IN_VMEM,
        scratch_shapes=[pltpu.SemaphoreType.DMA(())],
        cost_estimate=pl.CostEstimate(flops=0, bytes_accessed=4 * source.shape[0] * width, transcendentals=0),
        name="own_columns",
    )(index.reshape(1), source)


def out_kernel(place, *refs, chunk, seqs, blocks_of):
    pieces = refs[: place.shape[0]]
    latents = refs[place.shape[0] : place.shape[0] + len(blocks_of)]
    weight, keep, send, value, every, heads_in = refs[place.shape[0] + len(blocks_of) :]
    own_rank = pieces[0].shape[0]
    for j, piece in enumerate(pieces):
        rows = pl.ds(pl.multiple_of(place[j] * own_rank, own_rank), own_rank)
        value[rows, :] = piece[...]
    own_heads = every.shape[0]
    for latent, blocks in zip(latents, blocks_of):
        count = latent.shape[0]
        product = jnp.dot(latent[...], value[...], preferred_element_type=jnp.float32)
        for h in range(own_heads):
            columns = slice(h * VH, (h + 1) * VH)
            every[h, :count, :] = product[:, columns]
            for i, block in enumerate(blocks):
                heads_in[block * seqs : (block + 1) * seqs, columns] = every[
                    h, pl.ds(i * seqs * own_heads + h, seqs, own_heads), :
                ]
    rows_in = heads_in[...].astype(jnp.bfloat16)
    half = keep.shape[0]

    @pl.loop(0, keep.shape[1] // chunk)
    def _(i):
        part = pl.ds(pl.multiple_of(i * chunk, chunk), chunk)
        result = jnp.dot(rows_in, weight[:, part], preferred_element_type=jnp.float32)
        keep[:, part] = result[:half]
        send[:, part] = result[half:].astype(send.dtype)


def out_proj(place, pieces, latents, blocks_of, w_out, seqs):
    depth, width = w_out.shape
    rank = latents[0].shape[1]
    rows = seqs * sum(len(blocks) for blocks in blocks_of)
    return pl.pallas_call(
        functools.partial(
            out_kernel, chunk=chunk_of(width, 3584), seqs=seqs, blocks_of=blocks_of
        ),
        out_shape=(
            jax.ShapeDtypeStruct((rows // 2, width), jnp.float32),
            jax.ShapeDtypeStruct((rows // 2, width), jnp.bfloat16),
        ),
        in_specs=[IN_SMEM] + [IN_VMEM] * (len(pieces) + len(latents) + 1),
        out_specs=(IN_VMEM, IN_VMEM),
        scratch_shapes=[
            pltpu.VMEM((rank, depth), jnp.bfloat16),
            pltpu.VMEM((depth // VH, latents[0].shape[0], VH), jnp.float32),
            pltpu.VMEM((rows, depth), jnp.float32),
        ],
        compiler_params=pltpu.CompilerParams(vmem_limit_bytes=12 * MIB),
        cost_estimate=pl.CostEstimate(
            flops=2 * rows * width * depth,
            bytes_accessed=2 * depth * width,
            transcendentals=0,
        ),
        name="out_proj",
    )(place, *pieces, *latents, w_out)


def mlp_kernel(
    own_low, own_high, other_low, other_high, gate, up_hbm, down_hbm,
    keep_low, keep_high, send,
    up, down, gate_sum, up_sum, active, sems, *, chunk
):
    half, middle = own_low.shape
    count = middle // chunk

    def part(i):
        return pl.ds(pl.multiple_of(i * chunk, chunk), chunk)

    def up_copy(i):
        return pltpu.make_async_copy(up_hbm.at[:, part(i)], up.at[:, part(i)], sems.at[0, i])

    def down_copy(i):
        return pltpu.make_async_copy(down_hbm.at[:, part(i)], down.at[:, part(i)], sems.at[1, i])

    @pl.loop(0, 2 * count)
    def _(i):
        up_copy(i).start()

    @pl.loop(0, 2 * count)
    def _(i):
        down_copy(i).start()

    sides = ((own_low, other_low), (own_high, other_high))
    for weight, total in ((gate, gate_sum), (up, up_sum)):
        total[...] = jnp.zeros_like(total)
        for side, (own, other) in enumerate(sides):

            @pl.loop(0, count)
            def _(i):
                rows = jnp.concatenate([own[:, part(i)], other[:, part(i)]], axis=0)
                if weight is up:
                    up_copy(i + side * count).wait()
                total[...] += lax.dot_general(
                    weight[:, part(i + side * count)],
                    rows,
                    NT,
                    preferred_element_type=jnp.float32,
                )

    value = gate_sum[...]
    active[...] = (value / (1.0 + jnp.exp(-value)) * up_sum[...]).T.astype(jnp.bfloat16)
    for side, keep in enumerate((keep_low, keep_high)):

        @pl.loop(0, count)
        def _(i):
            down_copy(i + side * count).wait()
            columns = part(i + side * count)
            result = jnp.dot(active[...], down[:, columns], preferred_element_type=jnp.float32)
            keep[:, part(i)] = result[:half].astype(keep.dtype)
            send[:, columns] = result[half:].astype(send.dtype)


def gated_mlp(own, other, gate_rows, up_rows, w_down):
    half, middle = own[0].shape
    hidden, width = w_down.shape
    return pl.pallas_call(
        functools.partial(mlp_kernel, chunk=chunk_of(middle, 1792)),
        out_shape=(
            jax.ShapeDtypeStruct((half, middle), jnp.float32),
            jax.ShapeDtypeStruct((half, middle), jnp.float32),
            jax.ShapeDtypeStruct((half, width), jnp.bfloat16),
        ),
        in_specs=[IN_VMEM] * 5 + [IN_HBM] * 2,
        out_specs=(IN_VMEM,) * 3,
        scratch_shapes=[
            pltpu.VMEM((hidden, width), jnp.bfloat16),
            pltpu.VMEM((hidden, width), jnp.bfloat16),
            pltpu.VMEM((hidden, 2 * half), jnp.float32),
            pltpu.VMEM((hidden, 2 * half), jnp.float32),
            pltpu.VMEM((2 * half, hidden), jnp.bfloat16),
            pltpu.SemaphoreType.DMA((2, width // chunk_of(middle, 1792))),
        ],
        compiler_params=pltpu.CompilerParams(vmem_limit_bytes=38 * MIB),
        cost_estimate=pl.CostEstimate(
            flops=12 * half * width * hidden,
            bytes_accessed=6 * hidden * width,
            transcendentals=2 * half * hidden,
        ),
        name="gated_mlp",
    )(*own, *other, gate_rows, up_rows, w_down)


def direct_phases(rep_size, grp_size):
    out = []
    for axis, size, low in (("grp", grp_size, 2), ("rep", rep_size, 4)):
        bit = size
        while bit > low:
            ways = 4 if bit // 4 >= low else 2
            bit //= ways
            out.append((axis, size, bit, ways))
    return out


def gather_rows(rows, move, sizes):
    held = rows
    for axis, size, bit, ways in direct_phases(*sizes):
        held = jnp.concatenate([held] + [move(held, axis, bit * k) for k in range(1, ways)], axis=0)
    n, width = held.shape
    low, high = held[:, : width // 2], held[:, width // 2 :]
    low_x, high_y = move(low, "grp", 1), move(high, "rep", 2)
    low = jnp.concatenate([low, low_x], axis=0)
    wide = jnp.concatenate([high, high_y], axis=0)
    low_y, high_x = move(low, "rep", 2), move(wide, "grp", 1)
    low = jnp.concatenate([low, low_y], axis=0)
    high = jnp.concatenate([high, high_x[:n], high_y, high_x[n:]], axis=0)
    return (low, high), (move(low, "rep", 1), move(high, "rep", 1))


def scatter_sum(low, high, send, move, sizes):
    def add(mine, theirs):
        return mine + theirs.astype(jnp.float32)

    def narrow(value):
        return value.astype(jnp.bfloat16)

    middle = low.shape[1]
    n = low.shape[0] // 4
    got = move(send, "rep", 1)
    low, high = add(low, got[:, :middle]), add(high, got[:, middle:])
    low_got = move(narrow(low[2 * n :]), "rep", 2)
    high_got = move(narrow(jnp.concatenate([high[n : 2 * n], high[3 * n :]], axis=0)), "grp", 1)
    low = add(low[: 2 * n], low_got)
    high = add(jnp.concatenate([high[:n], high[2 * n : 3 * n]], axis=0), high_got)
    low_got, high_got = move(narrow(low[n:]), "grp", 1), move(narrow(high[n:]), "rep", 2)
    total = jnp.concatenate([add(low[:n], low_got), add(high[:n], high_got)], axis=1)
    for axis, size, bit, ways in reversed(direct_phases(*sizes)):
        per = total.shape[0] // ways
        moved = [
            move(narrow(total[k * per : (k + 1) * per]), axis, bit * k) for k in range(1, ways)
        ]
        total = total[:per]
        for piece in moved:
            total = add(total, piece)
    return total


def to_heads(near, far, move, sizes):
    got = move(far, "grp", 1)
    order = [phase for phase in direct_phases(*sizes) if phase[0] == "grp"]
    high = near.shape[0]
    held, senders = jnp.stack([near, got], axis=1), [0, high]
    if not order:
        return [held.reshape(-1, held.shape[-1])], (tuple(senders),)
    for n, (axis, size, bit, ways) in enumerate(order):
        per = held.shape[0] // ways
        weight = per
        parts = [held[k * per : (k + 1) * per] for k in range(ways)]
        parts = parts[:1] + [move(parts[k], axis, bit * k) for k in range(1, ways)]
        named = [[sender + k * weight for sender in senders] for k in range(ways)]
        if n + 1 < len(order):
            held, senders = jnp.concatenate(parts, axis=1), sum(named, [])
    return (
        [part.reshape(-1, part.shape[-1]) for part in parts],
        tuple(tuple(names) for names in named),
    )


def sum_heads(keep, send, move, sizes):
    got = move(send, "grp", 1)
    total = keep + got.astype(jnp.float32)
    for axis, size, bit, ways in [p for p in direct_phases(*sizes) if p[0] == "grp"]:
        per = total.shape[0] // ways
        moved = [
            move(total[k * per : (k + 1) * per].astype(jnp.bfloat16), axis, bit * k)
            for k in range(1, ways)
        ]
        total = total[:per]
        for piece in moved:
            total = total + piece.astype(jnp.float32)
    return total


def on_device(
    hidden_in,
    q_nope,
    q_rope,
    new_kv,
    cache_kv,
    lengths,
    w_uk,
    w_uv,
    w_out,
    norm_gain,
    w_gate,
    w_up,
    w_down,
    *,
    rep_size,
    grp_size,
):
    sizes = {"rep": rep_size, "grp": grp_size}

    def move(value, axis, bit):
        return lax.ppermute(value, axis, [(i, i ^ bit) for i in range(sizes[axis])])

    seqs, _ = hidden_in.shape
    heads = q_nope.shape[1] // NOPE
    rank_own = w_uk.shape[0]
    own_heads = heads // grp_size

    held = [q_nope]
    for step in range(1, rep_size):
        held.append(move(q_nope, "rep", step))
    held = jnp.concatenate(held, axis=0)
    q_part = jnp.einsum(
        "bhd,chd->bhc",
        held.reshape(seqs * rep_size, heads, NOPE),
        w_uk.reshape(rank_own, heads, NOPE),
        preferred_element_type=jnp.float32,
    ).astype(jnp.bfloat16)
    pieces = []
    for step in range(rep_size):
        piece = q_part[step * seqs : (step + 1) * seqs]
        pieces.append(move(piece, "rep", step) if step else piece)
    place = lax.axis_index("rep") ^ jnp.arange(rep_size, dtype=jnp.int32)

    values = [own_columns(w_uv, lax.axis_index("grp"), own_heads * VH)]
    for step in range(1, rep_size):
        low = step & -step
        values.append(move(values[step ^ low], "rep", low))

    near, far, out_weight = attend(
        lengths,
        place,
        lax.axis_index("grp").reshape(1),
        pieces,
        q_rope.reshape(seqs, heads, ROPE),
        new_kv,
        cache_kv,
        w_out,
        float(NOPE + ROPE) ** (-0.5),
        grp_size,
    )
    latents, blocks_of = to_heads(near, far, move, (rep_size, grp_size))
    keep, send = out_proj(place, values, latents, blocks_of, out_weight, seqs)
    attn_out = sum_heads(keep, send, move, (rep_size, grp_size))
    resid = (hidden_in.astype(jnp.float32) + attn_out).astype(jnp.bfloat16)
    resid_f32 = resid.astype(jnp.float32)
    mean_sq = jnp.mean(resid_f32 * resid_f32, axis=1, keepdims=True)
    normed = (
        resid_f32 * lax.rsqrt(mean_sq + epsilon) * norm_gain.astype(jnp.float32)
    ).astype(jnp.bfloat16)

    own, other = gather_rows(normed, move, (rep_size, grp_size))
    low, high, send = gated_mlp(own, other, w_gate.T, w_up.T, w_down)
    mlp_out = scatter_sum(low, high, send, move, (rep_size, grp_size))
    return (resid_f32 + mlp_out).astype(jnp.bfloat16)


def solution(mesh):
    def body(*args):
        return on_device(*args, rep_size=mesh.shape["rep"], grp_size=mesh.shape["grp"])

    return jax.shard_map(
        body,
        mesh=mesh,
        in_specs=(
            P(AXES, None),
            P(AXES, None),
            P(AXES, None),
            P(AXES, None),
            P(AXES, None, None),
            P(AXES),
            P("rep", None),
            P("rep", None),
            P("grp", None),
            P(),
            P(None, AXES),
            P(None, AXES),
            P(AXES, None),
        ),
        out_specs=P(AXES, None),
        check_vma=False,
    )
```

```python
import functools

import jax
import jax.numpy as jnp
from jax import lax
from jax.experimental import pallas as pl
from jax.experimental.pallas import tpu as pltpu
from jax.sharding import PartitionSpec as P


NOPE = 128
ROPE = 64
VH = 128

AXES = ("rep", "grp")
epsilon = 1e-06


MIB = 1024 * 1024
IN_HBM = pl.BlockSpec(memory_space=pltpu.HBM)
IN_VMEM = pl.BlockSpec(memory_space=pltpu.VMEM)
IN_SMEM = pl.BlockSpec(memory_space=pltpu.SMEM)
NT = (((1,), (1,)), ((), ()))


def chunk_of(size, wanted):
    chunk = wanted
    while size % chunk:
        chunk //= 2
    return chunk


def attend_kernel(lengths, place, group, *refs, chunk, scale, whole):
    pieces = refs[: place.shape[0]]
    (
        q_rope, new_kv, cache_hbm, weight_hbm, near, far, weight, cache, queries, scores, total,
        sems, weight_sems,
    ) = refs[place.shape[0] :]
    weight_rows = weight.shape[0] // weight_sems.shape[0]
    weight_copies = [
        pltpu.make_async_copy(
            weight_hbm.at[pl.ds(i * weight_rows, weight_rows)],
            weight.at[pl.ds(i * weight_rows, weight_rows)],
            weight_sems.at[i],
        )
        for i in range(weight_sems.shape[0])
    ]
    seqs, heads, own_rank = pieces[0].shape
    rank = own_rank * len(pieces)

    def part(i):
        return pl.ds(pl.multiple_of(i * chunk, chunk), chunk)

    def used(b):
        return (lengths[b] + (chunk - 1)) // chunk

    def copy(b, i):
        return pltpu.make_async_copy(
            cache_hbm.at[b, :, part(i)], cache.at[b, :, part(i)], sems.at[b, i]
        )

    for b in range(seqs):

        @pl.loop(0, used(b))
        def _(i):
            copy(b, i).start()

    for weight_copy in weight_copies:
        weight_copy.start()

    for b in range(seqs):
        for j, piece in enumerate(pieces):
            columns = pl.ds(pl.multiple_of(place[j] * own_rank, own_rank), own_rank)
            queries[b, :, columns] = piece[b]
        queries[b, :, rank:] = q_rope[b]

    steps = used(0)
    for b in range(1, seqs):
        steps = steps + used(b)
    copy(0, 0).wait()
    scores[0] = jnp.dot(queries[0], cache[0, :, part(0)], preferred_element_type=jnp.float32)

    def step(t, carry):
        b, i, top, denom = carry
        slot = t & 1
        last = i + 1 == used(b)
        next_b = jnp.where(last, b + 1, b)
        next_i = jnp.where(last, 0, i + 1)

        @pl.when(t + 1 < steps)
        def _():
            copy(next_b, next_i).wait()

        ahead_b = jnp.minimum(next_b, seqs - 1)
        first = i == 0
        own = new_kv[b].astype(jnp.float32)
        own_score = jnp.sum(queries[b].astype(jnp.float32) * own, axis=1, keepdims=True)
        top = jnp.where(first, own_score, top)
        denom = jnp.where(first, 1.0, denom)
        ahead = jnp.dot(
            queries[ahead_b], cache[ahead_b, :, part(next_i)], preferred_element_type=jnp.float32
        )
        position = i * chunk + lax.broadcasted_iota(jnp.int32, (1, chunk), 1)
        raw = scores[slot] + jnp.where(position < lengths[b], 0.0, -jnp.inf)
        new_top = jnp.maximum(top, jnp.max(raw, axis=1, keepdims=True))
        weights = jnp.exp((raw - new_top) * scale)
        shrink = jnp.exp((top - new_top) * scale)
        denom = denom * shrink + jnp.sum(weights, axis=1, keepdims=True)
        before = jnp.where(first, jnp.broadcast_to(own[:, :rank], (heads, rank)), total[...])
        fresh = before * shrink + lax.dot_general(
            weights.astype(jnp.bfloat16),
            cache[b, :rank, part(i)],
            NT,
            preferred_element_type=jnp.float32,
        )
        scores[1 - slot] = ahead
        total[...] = fresh

        @pl.when(last)
        def _():
            if whole:
                near[b] = (fresh / denom).astype(near.dtype)
                return
            total[...] = fresh / denom
            own_heads = heads // (2 * near.shape[0])
            place_rows = pl.ds(pl.multiple_of(b * own_heads, own_heads), own_heads)
            for x, block in enumerate((near, far)):
                for high in range(near.shape[0]):
                    first_head = (group[0] ^ (2 * high + x)) * own_heads
                    rows = pl.ds(pl.multiple_of(first_head, own_heads), own_heads)
                    block[high, place_rows, :] = total[rows, :].astype(block.dtype)

        return next_b, next_i, new_top, denom

    zero = jnp.zeros((heads, 1), jnp.float32)
    lax.fori_loop(0, steps, step, (jnp.int32(0), jnp.int32(0), zero, zero))
    for weight_copy in weight_copies:
        weight_copy.wait()


def attend(
    lengths, place, group, pieces, q_rope, new_kv, cache_kv, w_out, scale, grp_size
):
    seqs, heads, own_rank = pieces[0].shape
    rank = own_rank * len(pieces)
    capacity, depth = cache_kv.shape[1:]
    chunk = chunk_of(capacity, 1024)
    own_heads = heads // grp_size
    whole = own_heads % 8 != 0
    shapes = [(grp_size // 2, seqs * own_heads, rank)] * 2
    if whole:
        shapes = [(seqs, heads, rank), (8, 128)]
    blocks = [jax.ShapeDtypeStruct(shape, jnp.bfloat16) for shape in shapes]
    near, far, out_weight = pl.pallas_call(
        functools.partial(attend_kernel, chunk=chunk, scale=scale, whole=whole),
        out_shape=(*blocks, jax.ShapeDtypeStruct(w_out.shape, w_out.dtype)),
        in_specs=[IN_SMEM] * 3 + [IN_VMEM] * (len(pieces) + 2) + [IN_HBM] * 2,
        out_specs=(IN_VMEM,) * 3,
        scratch_shapes=[
            pltpu.VMEM((seqs, depth, capacity), jnp.bfloat16),
            pltpu.VMEM((seqs, heads, depth), jnp.bfloat16),
            pltpu.VMEM((2, heads, chunk), jnp.float32),
            pltpu.VMEM((heads, rank), jnp.float32),
            pltpu.SemaphoreType.DMA((seqs, capacity // chunk)),
            pltpu.SemaphoreType.DMA((4,)),
        ],
        compiler_params=pltpu.CompilerParams(vmem_limit_bytes=30 * MIB),
        cost_estimate=pl.CostEstimate(
            flops=4 * seqs * heads * capacity * depth,
            bytes_accessed=2 * seqs * capacity * depth,
            transcendentals=seqs * heads * capacity,
        ),
        name="attend",
    )(lengths, place, group, *pieces, q_rope, new_kv[:, None, :], cache_kv.transpose(0, 2, 1), w_out)
    if whole:
        latent = near.reshape(seqs, grp_size, own_heads, rank).swapaxes(0, 1)
        latent = latent.reshape(grp_size, seqs * own_heads, rank)
        latent = jnp.take(latent, group[0] ^ jnp.arange(grp_size), axis=0)
        near, far = latent[0::2], latent[1::2]
    return near, far, out_weight


def slice_kernel(start, source, out, sem):
    width = out.shape[1]
    columns = pl.ds(pl.multiple_of(start[0] * width, width), width)
    copy = pltpu.make_async_copy(source.at[:, columns], out, sem)
    copy.start()
    copy.wait()


def own_columns(source, index, width):
    return pl.pallas_call(
        slice_kernel,
        out_shape=jax.ShapeDtypeStruct((source.shape[0], width), source.dtype),
        in_specs=[IN_SMEM, IN_HBM],
        out_specs=IN_VMEM,
        scratch_shapes=[pltpu.SemaphoreType.DMA(())],
        cost_estimate=pl.CostEstimate(flops=0, bytes_accessed=4 * source.shape[0] * width, transcendentals=0),
        name="own_columns",
    )(index.reshape(1), source)


def out_kernel(place, *refs, chunk, seqs, blocks_of):
    pieces = refs[: place.shape[0]]
    latents = refs[place.shape[0] : place.shape[0] + len(blocks_of)]
    weight, keep, send, value, every, heads_in = refs[place.shape[0] + len(blocks_of) :]
    own_rank = pieces[0].shape[0]
    for j, piece in enumerate(pieces):
        rows = pl.ds(pl.multiple_of(place[j] * own_rank, own_rank), own_rank)
        value[rows, :] = piece[...]
    own_heads = every.shape[0]
    for latent, blocks in zip(latents, blocks_of):
        count = latent.shape[0]
        product = jnp.dot(latent[...], value[...], preferred_element_type=jnp.float32)
        for h in range(own_heads):
            columns = slice(h * VH, (h + 1) * VH)
            every[h, :count, :] = product[:, columns]
            for i, block in enumerate(blocks):
                heads_in[block * seqs : (block + 1) * seqs, columns] = every[
                    h, pl.ds(i * seqs * own_heads + h, seqs, own_heads), :
                ]
    rows_in = heads_in[...].astype(jnp.bfloat16)
    half = keep.shape[0]

    @pl.loop(0, keep.shape[1] // chunk)
    def _(i):
        part = pl.ds(pl.multiple_of(i * chunk, chunk), chunk)
        result = jnp.dot(rows_in, weight[:, part], preferred_element_type=jnp.float32)
        keep[:, part] = result[:half]
        send[:, part] = result[half:].astype(send.dtype)


def out_proj(place, pieces, latents, blocks_of, w_out, seqs):
    depth, width = w_out.shape
    rank = latents[0].shape[1]
    rows = seqs * sum(len(blocks) for blocks in blocks_of)
    return pl.pallas_call(
        functools.partial(
            out_kernel, chunk=chunk_of(width, 3584), seqs=seqs, blocks_of=blocks_of
        ),
        out_shape=(
            jax.ShapeDtypeStruct((rows // 2, width), jnp.float32),
            jax.ShapeDtypeStruct((rows // 2, width), jnp.bfloat16),
        ),
        in_specs=[IN_SMEM] + [IN_VMEM] * (len(pieces) + len(latents) + 1),
        out_specs=(IN_VMEM, IN_VMEM),
        scratch_shapes=[
            pltpu.VMEM((rank, depth), jnp.bfloat16),
            pltpu.VMEM((depth // VH, latents[0].shape[0], VH), jnp.float32),
            pltpu.VMEM((rows, depth), jnp.float32),
        ],
        compiler_params=pltpu.CompilerParams(vmem_limit_bytes=12 * MIB),
        cost_estimate=pl.CostEstimate(
            flops=2 * rows * width * depth,
            bytes_accessed=2 * depth * width,
            transcendentals=0,
        ),
        name="out_proj",
    )(place, *pieces, *latents, w_out)


def mlp_kernel(
    own_low, own_high, other_low, other_high, gate, up_hbm, down_hbm,
    keep_low, keep_high, send,
    up, down, gate_sum, up_sum, active, sems, *, chunk
):
    half, middle = own_low.shape
    count = middle // chunk

    def part(i):
        return pl.ds(pl.multiple_of(i * chunk, chunk), chunk)

    def up_copy(i):
        return pltpu.make_async_copy(up_hbm.at[:, part(i)], up.at[:, part(i)], sems.at[0, i])

    def down_copy(i):
        return pltpu.make_async_copy(down_hbm.at[:, part(i)], down.at[:, part(i)], sems.at[1, i])

    @pl.loop(0, 2 * count)
    def _(i):
        up_copy(i).start()

    @pl.loop(0, 2 * count)
    def _(i):
        down_copy(i).start()

    sides = ((own_low, other_low), (own_high, other_high))
    for weight, total in ((gate, gate_sum), (up, up_sum)):
        total[...] = jnp.zeros_like(total)
        for side, (own, other) in enumerate(sides):

            @pl.loop(0, count)
            def _(i):
                rows = jnp.concatenate([own[:, part(i)], other[:, part(i)]], axis=0)
                if weight is up:
                    up_copy(i + side * count).wait()
                total[...] += lax.dot_general(
                    weight[:, part(i + side * count)],
                    rows,
                    NT,
                    preferred_element_type=jnp.float32,
                )

    value = gate_sum[...]
    active[...] = (value / (1.0 + jnp.exp(-value)) * up_sum[...]).T.astype(jnp.bfloat16)
    for side, keep in enumerate((keep_low, keep_high)):

        @pl.loop(0, count)
        def _(i):
            down_copy(i + side * count).wait()
            columns = part(i + side * count)
            result = jnp.dot(active[...], down[:, columns], preferred_element_type=jnp.float32)
            keep[:, part(i)] = result[:half].astype(keep.dtype)
            send[:, columns] = result[half:].astype(send.dtype)


def gated_mlp(own, other, gate_rows, up_rows, w_down):
    half, middle = own[0].shape
    hidden, width = w_down.shape
    return pl.pallas_call(
        functools.partial(mlp_kernel, chunk=chunk_of(middle, 1792)),
        out_shape=(
            jax.ShapeDtypeStruct((half, middle), jnp.float32),
            jax.ShapeDtypeStruct((half, middle), jnp.float32),
            jax.ShapeDtypeStruct((half, width), jnp.bfloat16),
        ),
        in_specs=[IN_VMEM] * 5 + [IN_HBM] * 2,
        out_specs=(IN_VMEM,) * 3,
        scratch_shapes=[
            pltpu.VMEM((hidden, width), jnp.bfloat16),
            pltpu.VMEM((hidden, width), jnp.bfloat16),
            pltpu.VMEM((hidden, 2 * half), jnp.float32),
            pltpu.VMEM((hidden, 2 * half), jnp.float32),
            pltpu.VMEM((2 * half, hidden), jnp.bfloat16),
            pltpu.SemaphoreType.DMA((2, width // chunk_of(middle, 1792))),
        ],
        compiler_params=pltpu.CompilerParams(vmem_limit_bytes=38 * MIB),
        cost_estimate=pl.CostEstimate(
            flops=12 * half * width * hidden,
            bytes_accessed=6 * hidden * width,
            transcendentals=2 * half * hidden,
        ),
        name="gated_mlp",
    )(*own, *other, gate_rows, up_rows, w_down)


def direct_phases(rep_size, grp_size):
    out = []
    for axis, size, low in (("grp", grp_size, 2), ("rep", rep_size, 4)):
        bit = size
        while bit > low:
            ways = 4 if bit // 4 >= low else 2
            bit //= ways
            out.append((axis, size, bit, ways))
    return out


def gather_rows(rows, move, sizes):
    def named(k, value, axis, bit):
        return move(value, axis, bit * k)

    held = rows
    for axis, size, bit, ways in direct_phases(*sizes):
        others = [named(k, held, axis, bit) for k in range(1, ways)]
        held = jnp.concatenate([held] + others, axis=0)
    n, width = held.shape
    low, high = held[:, : width // 2], held[:, width // 2 :]
    low_x, high_y = move(low, "grp", 1), move(high, "rep", 2)
    low = jnp.concatenate([low, low_x], axis=0)
    wide = jnp.concatenate([high, high_y], axis=0)
    low_y, high_x = move(low, "rep", 2), move(wide, "grp", 1)
    low = jnp.concatenate([low, low_y], axis=0)
    high = jnp.concatenate([high, high_x[:n], high_y, high_x[n:]], axis=0)
    return (low, high), (move(low, "rep", 1), move(high, "rep", 1))


def scatter_sum(low, high, send, move, sizes):
    def named(k, value, axis, bit):
        return move(value, axis, bit * k)


    def add(mine, theirs):
        return mine + theirs.astype(jnp.float32)

    def narrow(value):
        return value.astype(jnp.bfloat16)

    middle = low.shape[1]
    n = low.shape[0] // 4
    got = move(send, "rep", 1)
    low, high = add(low, got[:, :middle]), add(high, got[:, middle:])
    low_got = move(narrow(low[2 * n :]), "rep", 2)
    high_got = move(narrow(jnp.concatenate([high[n : 2 * n], high[3 * n :]], axis=0)), "grp", 1)
    low = add(low[: 2 * n], low_got)
    high = add(jnp.concatenate([high[:n], high[2 * n : 3 * n]], axis=0), high_got)
    low_got, high_got = move(narrow(low[n:]), "grp", 1), move(narrow(high[n:]), "rep", 2)
    total = jnp.concatenate([add(low[:n], low_got), add(high[:n], high_got)], axis=1)
    for axis, size, bit, ways in reversed(direct_phases(*sizes)):
        per = total.shape[0] // ways
        moved = [
            named(k, narrow(total[k * per : (k + 1) * per]), axis, bit)
            for k in range(1, ways)
        ]
        total = total[:per]
        for piece in moved:
            total = add(total, piece)
    return total


def to_heads(near, far, move, sizes):
    def named(k, value, axis, bit):
        return move(value, axis, bit * k)

    got = move(far, "grp", 1)
    order = [phase for phase in direct_phases(*sizes) if phase[0] == "grp"]
    high = near.shape[0]
    held, senders = jnp.stack([near, got], axis=1), [0, high]
    if not order:
        return [held.reshape(-1, held.shape[-1])], (tuple(senders),)
    for n, (axis, size, bit, ways) in enumerate(order):
        per = held.shape[0] // ways
        weight = per
        parts = [held[k * per : (k + 1) * per] for k in range(ways)]
        parts = parts[:1] + [named(k, parts[k], axis, bit) for k in range(1, ways)]
        places = [[sender + k * weight for sender in senders] for k in range(ways)]
        if n + 1 < len(order):
            held, senders = jnp.concatenate(parts, axis=1), sum(places, [])
    return (
        [part.reshape(-1, part.shape[-1]) for part in parts],
        tuple(tuple(names) for names in places),
    )


def sum_heads(keep, send, move, sizes):
    def named(k, value, axis, bit):
        return move(value, axis, bit * k)

    got = move(send, "grp", 1)
    total = keep + got.astype(jnp.float32)
    for axis, size, bit, ways in [p for p in direct_phases(*sizes) if p[0] == "grp"]:
        per = total.shape[0] // ways
        moved = [
            named(k, total[k * per : (k + 1) * per].astype(jnp.bfloat16), axis, bit)
            for k in range(1, ways)
        ]
        total = total[:per]
        for piece in moved:
            total = total + piece.astype(jnp.float32)
    return total


def on_device(
    hidden_in,
    q_nope,
    q_rope,
    new_kv,
    cache_kv,
    lengths,
    w_uk,
    w_uv,
    w_out,
    norm_gain,
    w_gate,
    w_up,
    w_down,
    *,
    rep_size,
    grp_size,
):
    sizes = {"rep": rep_size, "grp": grp_size}

    def move(value, axis, bit):
        return lax.ppermute(value, axis, [(i, i ^ bit) for i in range(sizes[axis])])

    seqs, _ = hidden_in.shape
    heads = q_nope.shape[1] // NOPE
    rank_own = w_uk.shape[0]
    own_heads = heads // grp_size

    held = [q_nope]
    for step in range(1, rep_size):
        held.append(move(q_nope, "rep", step))
    held = jnp.concatenate(held, axis=0)
    q_part = jnp.einsum(
        "bhd,chd->bhc",
        held.reshape(seqs * rep_size, heads, NOPE),
        w_uk.reshape(rank_own, heads, NOPE),
        preferred_element_type=jnp.float32,
    ).astype(jnp.bfloat16)
    pieces = []
    for step in range(rep_size):
        piece = q_part[step * seqs : (step + 1) * seqs]
        pieces.append(move(piece, "rep", step) if step else piece)
    place = lax.axis_index("rep") ^ jnp.arange(rep_size, dtype=jnp.int32)

    values = [own_columns(w_uv, lax.axis_index("grp"), own_heads * VH)]
    for step in range(1, rep_size):
        low = step & -step
        values.append(move(values[step ^ low], "rep", low))

    near, far, out_weight = attend(
        lengths,
        place,
        lax.axis_index("grp").reshape(1),
        pieces,
        q_rope.reshape(seqs, heads, ROPE),
        new_kv,
        cache_kv,
        w_out,
        float(NOPE + ROPE) ** (-0.5),
        grp_size,
    )
    latents, blocks_of = to_heads(near, far, move, (rep_size, grp_size))
    keep, send = out_proj(place, values, latents, blocks_of, out_weight, seqs)
    attn_out = sum_heads(keep, send, move, (rep_size, grp_size))
    resid = (hidden_in.astype(jnp.float32) + attn_out).astype(jnp.bfloat16)
    resid_f32 = resid.astype(jnp.float32)
    mean_sq = jnp.mean(resid_f32 * resid_f32, axis=1, keepdims=True)
    normed = (
        resid_f32 * lax.rsqrt(mean_sq + epsilon) * norm_gain.astype(jnp.float32)
    ).astype(jnp.bfloat16)

    own, other = gather_rows(normed, move, (rep_size, grp_size))
    low, high, send = gated_mlp(own, other, w_gate.T, w_up.T, w_down)
    mlp_out = scatter_sum(low, high, send, move, (rep_size, grp_size))
    return (resid_f32 + mlp_out).astype(jnp.bfloat16)


def solution(mesh):
    def body(*args):
        return on_device(*args, rep_size=mesh.shape["rep"], grp_size=mesh.shape["grp"])

    return jax.shard_map(
        body,
        mesh=mesh,
        in_specs=(
            P(AXES, None),
            P(AXES, None),
            P(AXES, None),
            P(AXES, None),
            P(AXES, None, None),
            P(AXES),
            P("rep", None),
            P("rep", None),
            P("grp", None),
            P(),
            P(None, AXES),
            P(None, AXES),
            P(AXES, None),
        ),
        out_specs=P(AXES, None),
        check_vma=False,
    )
```
